256 devices in a mesh: seq: 16 (over y, z_lo), expert: 8 (over x, core), batch: 2 (over z_hi).
Axes of the slice: x: 4, y: 4, z: 8 (z_hi: 2, z_lo: 4; z = z_hi * 4 + z_lo), core: 2. Of those that a mesh axis runs over, the one named last changes fastest.
Arguments:
- hidden_state: bfloat16 [64, 4096], P(('batch', 'expert'), 'seq'), may hold values from -9 to 9
- queries: bfloat16 [64, 2048], P(('batch', 'expert'), 'seq'), may hold values from -180 to 180
- page_table: int32 [64, 16, 4], P(('batch', 'expert'), 'seq'), may hold values from 0 to 19, as said below
- lengths: int32 [64], P(('batch', 'expert')), may hold values from 2048 to 8192
- paged_keys: bfloat16 [16, 320, 128, 512], P(('batch', 'expert'), 'seq'), may hold values from -6 to 6
- paged_values: bfloat16 [16, 320, 128, 512], P(('batch', 'expert'), 'seq'), may hold values from -6 to 6
- out_weight: bfloat16 [2048, 4096], P('seq', 'expert'), may hold values from -1.5 to 1.5
- norm_gain: float32 [4096], P('seq'), may hold values from 0.25 to 1.75
- expert_ids: int32 [64, 2], P(('batch', 'expert')), may hold values from 0 to 7, all different within a row; in each aligned block of 4 rows (0 to 3, 4 to 7, ...) at most 2 rows name the same one
- route_weights: float32 [64, 2], P(('batch', 'expert')), may hold values from 0.25 to 1
- expert_gate: bfloat16 [8, 4096, 8192], P('expert', None, ('seq', 'batch')), may hold values from -0.09375 to 0.09375
- expert_up: bfloat16 [8, 4096, 8192], P('expert', None, ('seq', 'batch')), may hold values from -0.09375 to 0.09375
- expert_down: bfloat16 [8, 8192, 4096], P('expert', ('seq', 'batch')), may hold values from -0.0625 to 0.0625
Outputs:
- layer_out: bfloat16 [64, 4096], P(('batch', 'expert'), 'seq')
The draws below stay inside these ranges and needn't reach their ends.
Inputs may be any that keep to these rules, and one draw needn't show every extreme that they name: `page_table`: the page ids of one block's sequences on one shard are all different. `expert_ids`: a token's two experts differ; within the 4 rows of one device no expert is named more than 2 times.
All inputs are finite; a program needn't handle non-finite values.
Results may differ from the reference program's by a relative error of at most 0.006.
Values may be sent and summed in bfloat16 or wider, within the bound.
A program may use at most 64 MiB of HBM per device.

```python
import math
import jax
import jax.numpy as jnp
import numpy as np
from jax import lax

D = 4096
QUERY_HEADS = 16
KEY_VALUE_HEADS = 4
HEAD_DIM = 128
FF_WIN = 8192
PAGE_TOKENS = 128
SEQUENCE_SLOTS = 4
SEQ_DEV = 4
DEVICE_COUNT = 16
EXPERTS = 8
SEQUENCE_BLOCKS = 16
BATCH = 64
POOL_PAGES = 20
CAP = 2


def table_from(key):
    device_keys = jax.random.split(key, SEQUENCE_BLOCKS * DEVICE_COUNT)

    def one_device(device_key):
        return jax.random.permutation(device_key, POOL_PAGES)[:SEQ_DEV * SEQUENCE_SLOTS].reshape(SEQ_DEV, SEQUENCE_SLOTS)
    page_tables = jax.vmap(one_device)(device_keys).reshape(SEQUENCE_BLOCKS, DEVICE_COUNT, SEQ_DEV, SEQUENCE_SLOTS)
    return jnp.transpose(page_tables, (0, 2, 1, 3)).reshape(SEQUENCE_BLOCKS * SEQ_DEV, DEVICE_COUNT, SEQUENCE_SLOTS).astype(jnp.int32)


def keys_from(key):
    start_offset = jnp.clip(jax.random.normal(key, (SEQUENCE_BLOCKS, DEVICE_COUNT * POOL_PAGES, PAGE_TOKENS, KEY_VALUE_HEADS * HEAD_DIM), jnp.float32), -6.0, 6.0)
    return start_offset


def draw_page_table(key, part):
    return table_from(jax.random.fold_in(key, 12))


def draw_paged_keys(key, part):
    return keys_from(jax.random.fold_in(key, 11)).astype(jnp.bfloat16)


def draw_queries(key, part):
    row_tally = SEQUENCE_BLOCKS * SEQ_DEV
    drawn = jnp.clip(1.5 * jax.random.normal(jax.random.fold_in(key, 13), (row_tally, QUERY_HEADS * HEAD_DIM), jnp.float32), -9.0, 9.0)
    return drawn.astype(jnp.bfloat16)


def draw_hidden_state(key, part):
    row_tally = SEQUENCE_BLOCKS * SEQ_DEV
    ramp = 0.5 + jnp.arange(D, dtype=jnp.float32) / D
    start_offset = jax.random.normal(jax.random.fold_in(key, 22), (row_tally, D), jnp.float32)
    return jnp.clip(start_offset * ramp, -9.0, 9.0).astype(jnp.bfloat16)


def plant(drawn, stream_key, low, top_value):
    shape = drawn.shape
    spot = [jax.random.randint(jax.random.fold_in(stream_key, axis), (), 0, shape[axis]) for axis in range(len(shape))]
    drawn = drawn.at[tuple(spot)].set(low)
    longest = shape.index(max(shape))
    spot[longest] = (spot[longest] + 1) % shape[longest]
    return drawn.at[tuple(spot)].set(top_value)


def block_levels(stream_key, dims, cuts, least, largest):
    def one(position, shards_of):
        steps = jax.random.uniform(jax.random.fold_in(jax.random.fold_in(stream_key, 6), position), (shards_of,), jnp.float32, least / len(cuts), largest / len(cuts))
        return jnp.repeat(jnp.exp(steps), dims[position] // shards_of).reshape((-1,) + (1,) * (len(dims) - position - 1))

    gain = one(*cuts[0])
    for cut in cuts[1:]:
        gain = gain * one(*cut)
    return gain


def deal_out(rng, own, number, rows, amount, top, limit, skew):
    sequence = jax.random.permutation(rng, amount)
    crowded, ordinary = load_shares(amount, rows * top, limit, skew, True), load_shares(amount, rows * top, limit, skew, False)
    places = jnp.arange(amount)

    def named(sizes, offset_by):
        used = int((sizes > 0).sum())
        fixed = max(1, used // 4)
        shifted = fixed + (places - fixed + offset_by * (used - fixed)) % max(1, amount - fixed)
        return jnp.zeros((amount,), jnp.int32).at[sequence[jnp.where(places < fixed, places, shifted)]].set(jnp.asarray(sizes, jnp.int32))

    sizes = jnp.where(number % 4 == 0, named(crowded, number // 4), named(ordinary, number - number // 4 - 1))
    mixed = jax.random.permutation(jax.random.fold_in(own, 3), amount)
    giver, receiver = mixed[0:amount // 2 * 2:2], mixed[1:amount // 2 * 2:2]
    room = jnp.minimum(sizes[giver] - 1, limit - sizes[receiver]) // 2
    room = jnp.where((giver == sequence[0]) | (receiver == sequence[0]) | (sizes[receiver] == 0), 0, jnp.maximum(room, 0))
    shifted = jax.random.randint(jax.random.fold_in(own, 4), (amount // 2,), 0, 1 << 20) % (room + 1)
    sizes = sizes.at[giver].add(-shifted).at[receiver].add(shifted)
    members = jnp.searchsorted(jnp.cumsum(sizes), jnp.arange(rows * top), side="right").astype(jnp.int32)
    listing = members.reshape(top, rows).T
    listing = listing[jax.random.permutation(jax.random.fold_in(own, 1), rows)]
    offset_by = jax.random.randint(jax.random.fold_in(own, 2), (rows, 1), 0, top)
    return jnp.take_along_axis(listing, (jnp.arange(top)[None, :] + offset_by) % top, axis=1)


def load_shares(number_of, total, limit, slope, full):
    weights = [(1 << 20) // math.isqrt(rank ** slope) + 1 for rank in range(1, number_of + 1)]
    largest = limit if full else min(limit, max(-(-total // number_of), total * weights[0] // sum(weights)))
    least = 1 if total - largest >= number_of - 1 else 0
    counts, surplus = [largest] + [least] * (number_of - 1), total - largest - least * (number_of - 1)
    while surplus > 0:
        movable = [i for i in range(1, number_of) if counts[i] < largest] or [i for i in range(1, number_of) if counts[i] < limit]
        whole, remaining = sum([weights[i] for i in movable]), surplus
        for i in movable:
            more = min(limit - counts[i], max(1, remaining * weights[i] // whole), surplus)
            counts[i] = counts[i] + more
            surplus = surplus - more
    return np.array(counts)


def gaussian(own_key, extent, scale, most, cuts=(), kind=jnp.bfloat16):
    values = jax.random.normal(own_key, extent, jnp.float32) * scale
    if len(cuts) > 0:
        values = block_levels(own_key, extent, cuts, -0.22, 0.18) * values
    return jnp.clip(values, min=-most, max=most).astype(kind)


def setup_inputs(seed: int = 0) -> dict:
    arg_keys = jax.random.split(jax.random.key(seed), 14)
    hidden_state = draw_hidden_state(jax.random.fold_in(arg_keys[13], 71), 0)
    queries = draw_queries(jax.random.fold_in(arg_keys[13], 71), 0)
    page_table = draw_page_table(jax.random.fold_in(arg_keys[13], 71), 0)
    lengths = plant(jax.random.randint(arg_keys[3], (BATCH,), DEVICE_COUNT * PAGE_TOKENS, DEVICE_COUNT * SEQUENCE_SLOTS * PAGE_TOKENS + 1), jax.random.fold_in(arg_keys[3], 1), DEVICE_COUNT * PAGE_TOKENS, DEVICE_COUNT * SEQUENCE_SLOTS * PAGE_TOKENS).astype(jnp.int32)
    paged_keys = draw_paged_keys(jax.random.fold_in(arg_keys[13], 71), 0)
    paged_values = gaussian(arg_keys[5], (SEQUENCE_BLOCKS, DEVICE_COUNT * POOL_PAGES, PAGE_TOKENS, KEY_VALUE_HEADS * HEAD_DIM), 1.0, 6.0, ((0, 16), (1, 16)))
    out_weight = gaussian(arg_keys[6], (QUERY_HEADS * HEAD_DIM, D), (HEAD_DIM // 8) ** -0.5, 1.5, ((0, 16), (1, 8)))
    norm_gain = jnp.clip(1.0 + 0.15 * jax.random.normal(arg_keys[7], (D,), jnp.float32), 0.25, 1.75)
    expert_ids_keys = jax.random.split(jax.random.fold_in(arg_keys[8], 1), BATCH // SEQ_DEV)
    expert_ids_turns = jax.random.permutation(jax.random.fold_in(arg_keys[8], 3), BATCH // SEQ_DEV)
    expert_ids = jax.vmap(lambda own, number: deal_out(jax.random.fold_in(arg_keys[8], 2), own, number, SEQ_DEV, EXPERTS, 2, CAP, 2))(expert_ids_keys, expert_ids_turns).reshape((BATCH, 2))
    route_weights = jnp.clip(0.25 + 0.75 * jax.random.uniform(arg_keys[9], (BATCH, 2), jnp.float32) ** block_levels(arg_keys[9], (BATCH, 2), ((0, 16),), -0.2, 0.2), 0.25, 1.0)
    expert_gate = gaussian(arg_keys[10], (EXPERTS, D, FF_WIN), D ** -0.5, 0.09375, ((0, 8), (2, 32)))
    expert_up = gaussian(arg_keys[11], (EXPERTS, D, FF_WIN), D ** -0.5, 0.09375, ((0, 8), (2, 32)))
    expert_down = gaussian(arg_keys[12], (EXPERTS, FF_WIN, D), FF_WIN ** -0.5, 0.0625, ((0, 8), (1, 32)))
    return {"hidden_state": hidden_state, "queries": queries, "page_table": page_table, "lengths": lengths, "paged_keys": paged_keys, "paged_values": paged_values, "out_weight": out_weight, "norm_gain": norm_gain, "expert_ids": expert_ids, "route_weights": route_weights, "expert_gate": expert_gate, "expert_up": expert_up, "expert_down": expert_down}


def shard_partials(grouped_queries, keys_per_page, values_per_page, usable):
    local_rows, kv_heads, block_length, head_size = grouped_queries.shape
    scores = jnp.einsum('skgd,slkd->skgl', grouped_queries.astype(jnp.float32), keys_per_page.astype(jnp.float32)) / math.sqrt(head_size)
    scores = jnp.where(usable[:, None, None, :], scores, -1e+30)
    maxima = lax.optimization_barrier(jnp.max(scores, axis=-1))
    powers = jnp.exp(scores - maxima[..., None])
    totals = lax.optimization_barrier(jnp.sum(powers, axis=-1))
    weights = lax.optimization_barrier(powers.astype(jnp.bfloat16)).astype(jnp.float32)
    weighted = jnp.einsum('skgl,slkd->skgd', weights, values_per_page.astype(jnp.float32))
    heads_all = kv_heads * block_length
    return (maxima.reshape(local_rows, heads_all), totals.reshape(local_rows, heads_all), weighted.reshape(local_rows, heads_all, head_size))

def slot_table(expert_ids, expert_count, capacity):
    flat_ids = expert_ids.reshape(-1).astype(jnp.int32)
    ordinal = jnp.arange(flat_ids.shape[0], dtype=jnp.int32)
    before = (flat_ids[:, None] == flat_ids[None, :]) & (ordinal[None, :] < ordinal[:, None])
    slot_of = lax.optimization_barrier(jnp.sum(before.astype(jnp.int32), axis=1)).astype(jnp.int32)
    target = flat_ids * capacity + slot_of
    return jnp.arange(expert_count * capacity, dtype=jnp.int32)[:, None] == target[None, :]

def reference(hidden_state, queries, page_table, lengths, paged_keys, paged_values, out_weight, norm_gain, expert_ids, route_weights, expert_gate, expert_up, expert_down):
    block_length = QUERY_HEADS // KEY_VALUE_HEADS

    def one_sequence(sequence_number):
        block_number = sequence_number // SEQ_DEV
        rows_per_page = (jnp.arange(DEVICE_COUNT, dtype=jnp.int32)[:, None] * POOL_PAGES + page_table[sequence_number].astype(jnp.int32)).astype(jnp.int32)
        sequence_keys = paged_keys[block_number][rows_per_page].reshape(DEVICE_COUNT, SEQUENCE_SLOTS * PAGE_TOKENS, KEY_VALUE_HEADS, HEAD_DIM)
        sequence_values = paged_values[block_number][rows_per_page].reshape(DEVICE_COUNT, SEQUENCE_SLOTS * PAGE_TOKENS, KEY_VALUE_HEADS, HEAD_DIM)
        positions = ((jnp.arange(SEQUENCE_SLOTS, dtype=jnp.int32)[None, :, None] * DEVICE_COUNT + jnp.arange(DEVICE_COUNT, dtype=jnp.int32)[:, None, None]) * PAGE_TOKENS + jnp.arange(PAGE_TOKENS, dtype=jnp.int32)[None, None, :]).reshape(DEVICE_COUNT, SEQUENCE_SLOTS * PAGE_TOKENS)
        usable = positions < lengths[sequence_number]
        block_grouped = jnp.broadcast_to(queries[sequence_number].reshape(1, KEY_VALUE_HEADS, block_length, HEAD_DIM), (DEVICE_COUNT, KEY_VALUE_HEADS, block_length, HEAD_DIM))
        maxima, totals, weighted = shard_partials(block_grouped, sequence_keys, sequence_values, usable)
        joint_max = lax.optimization_barrier(jnp.max(maxima, axis=0))
        factor = jnp.exp(maxima - joint_max)
        summed = lax.optimization_barrier(jnp.sum(weighted * factor[..., None], axis=0)) / lax.optimization_barrier(jnp.sum(totals * factor, axis=0))[:, None]
        return summed.reshape(QUERY_HEADS * HEAD_DIM).astype(jnp.bfloat16)
    attention = lax.map(one_sequence, jnp.arange(BATCH, dtype=jnp.int32))
    projected = jnp.dot(attention, out_weight, preferred_element_type=jnp.float32)
    resid = hidden_state.astype(jnp.float32) + projected
    normed = (resid * lax.rsqrt(lax.optimization_barrier(jnp.mean(resid * resid, axis=1, keepdims=True)) + 1e-05) * norm_gain).astype(jnp.bfloat16)
    normed_groups = lax.optimization_barrier(normed).astype(jnp.float32).reshape(SEQUENCE_BLOCKS, SEQ_DEV, D)
    placed = jax.vmap(lambda block_ids: slot_table(block_ids, EXPERTS, CAP))(expert_ids.reshape(SEQUENCE_BLOCKS, SEQ_DEV, 2))
    placed = placed.reshape(SEQUENCE_BLOCKS, EXPERTS * CAP, SEQ_DEV, 2).astype(jnp.float32)
    dispatch = lax.optimization_barrier(jnp.sum(placed, axis=3))
    buffers = jnp.einsum('grs,gsd->grd', dispatch, normed_groups).astype(jnp.bfloat16)
    buffers = jnp.transpose(buffers.reshape(SEQUENCE_BLOCKS, EXPERTS, CAP, D), (1, 0, 2, 3)).reshape(EXPERTS, SEQUENCE_BLOCKS * CAP, D)

    def run_expert(operands):
        token_rows, gate_matrix, up_matrix, down_matrix = operands
        gate_part = jnp.dot(token_rows, gate_matrix, preferred_element_type=jnp.float32)
        up_part = jnp.dot(token_rows, up_matrix, preferred_element_type=jnp.float32)
        activated = (jax.nn.silu(gate_part) * up_part).astype(jnp.bfloat16)
        return jnp.dot(activated, down_matrix, preferred_element_type=jnp.float32)
    outputs = lax.map(run_expert, (buffers, expert_gate, expert_up, expert_down))
    outputs = jnp.transpose(outputs.reshape(EXPERTS, SEQUENCE_BLOCKS, CAP, D), (1, 0, 2, 3)).reshape(SEQUENCE_BLOCKS, EXPERTS * CAP, D)
    mixing = jnp.einsum('grsk,gsk->gsr', placed, route_weights.reshape(SEQUENCE_BLOCKS, SEQ_DEV, 2), precision=lax.Precision.HIGHEST)
    expert_mix = jnp.einsum('gsr,grd->gsd', mixing, outputs, precision=lax.Precision.HIGHEST).reshape(BATCH, D)
    return (resid + expert_mix).astype(jnp.bfloat16)
```

```python
import functools
import math

import jax
import jax.numpy as jnp
from jax import lax
from jax.experimental import pallas as pl
from jax.experimental.pallas import tpu as pltpu
from jax.sharding import PartitionSpec as P

D = 4096
QUERY_HEADS = 16
KEY_VALUE_HEADS = 4
HEAD_DIM = 128
PAGE_TOKENS = 128
SLOTS = 4
ROWS = 4
SEQ = 16
EXPERTS = 8
BATCHES = 2
POOL = 20
FEATURES = D // SEQ
HIDDEN = 256
QUARTER = D // 4
BF = jnp.bfloat16
F32 = jnp.float32
MESH = pl.DeviceIdType.MESH


def iota(shape, dim):
    return lax.broadcasted_iota(jnp.int32, shape, dim)


def kernel(
    hidden_ref, query_ref, table_ref, length_ref, keys_hbm, values_hbm, weight_hbm, gain_ref,
    ids_ref, route_ref, gate_hbm, up_hbm, down_hbm, out_ref,
    keys, values, gate, up, down, weights,
    query_buf, query_rows, part, part_buf, proj, proj_buf, info, slabs, tokens,
    sent, slots, returned, results, terms, term_buf,
    local_sems, send_sems, recv_sems,
):
    s = lax.axis_index("seq")
    e = lax.axis_index("expert")
    b = lax.axis_index("batch")
    me = b * SEQ + s

    local = [
        pltpu.make_async_copy(source, target, local_sems.at[k])
        for k, (source, target) in enumerate((
            (keys_hbm, keys), (values_hbm, values), (weight_hbm, weights.at[e]),
            (gate_hbm, gate), (up_hbm, up), (down_hbm, down),
        ))
    ]
    for copy in local:
        copy.start()

    def seq_peer(d):
        return lax.rem(s + d, SEQ)

    def expert_peer(d):
        return lax.rem(e + d, EXPERTS)

    def pair_peer(d):
        return lax.rem(me + d, BATCHES * SEQ)

    barrier = pltpu.get_barrier_semaphore()
    for d in range(1, SEQ):
        pl.semaphore_signal(barrier, 1, device_id={"seq": seq_peer(d)}, device_id_type=MESH)
    for d in range(1, EXPERTS):
        pl.semaphore_signal(barrier, 1, device_id={"expert": expert_peer(d)}, device_id_type=MESH)
    pl.semaphore_signal(barrier, 1, device_id={"batch": 1 - b}, device_id_type=MESH)

    ids = [[ids_ref[t, k] for k in range(2)] for t in range(ROWS)]
    row8, lane8 = iota((8, 128), 0), iota((8, 128), 1)
    slab = jnp.full((8, 128), -1.0, F32)
    for t in range(ROWS):
        for k in range(2):
            earlier = jnp.int32(0)
            for a in range(2 * t + k):
                earlier = earlier + jnp.where(ids[a // 2][a % 2] == ids[t][k], 1, 0)
            target = (ids[t][k] * 2 + earlier).astype(F32)
            slab = jnp.where((row8 == t) & (lane8 == k), target, slab)
            slab = jnp.where((row8 == t) & (lane8 == 2 + k), route_ref[t, k], slab)
    info[b] = slab
    tokens[...] = jnp.zeros_like(tokens)
    query_buf[s] = query_ref[...]

    pl.semaphore_wait(barrier, SEQ - 1 + EXPERTS - 1 + 1)

    def send(source, target, phase, device):
        pltpu.make_async_remote_copy(
            src_ref=source, dst_ref=target, send_sem=send_sems.at[phase],
            recv_sem=recv_sems.at[phase], device_id=device, device_id_type=MESH,
        ).start()

    def whole(ref, phase):
        return pltpu.make_async_remote_copy(
            src_ref=ref, dst_ref=ref, send_sem=send_sems.at[phase],
            recv_sem=recv_sems.at[phase], device_id={"batch": 1 - b}, device_id_type=MESH,
        )

    for d in range(1, SEQ):
        send(query_ref, query_buf.at[s], 0, {"seq": seq_peer(d)})
    send(info.at[b], info.at[b], 1, {"batch": 1 - b})
    for d in range(1, EXPERTS):
        send(weight_hbm, weights.at[e], 2, {"expert": expert_peer(d)})

    local[0].wait()
    local[1].wait()
    whole(query_buf.at[pl.ds(0, SEQ - 1)], 0).wait_recv()
    for h in range(QUERY_HEADS):
        query_rows[pl.ds(ROWS * h, ROWS), :] = query_buf[h].astype(F32)
    width = KEY_VALUE_HEADS * HEAD_DIM
    own_group = iota((QUERY_HEADS, width), 1) // HEAD_DIM == iota((QUERY_HEADS, width), 0) // 4
    spot = iota((QUERY_HEADS, SLOTS * PAGE_TOKENS), 1)
    position = (spot // PAGE_TOKENS * SEQ + s) * PAGE_TOKENS + spot % PAGE_TOKENS
    group_of = iota((QUERY_HEADS, HEAD_DIM), 0) // 4
    lane16 = iota((QUERY_HEADS, HEAD_DIM), 1)
    for i in range(ROWS):
        q = query_rows[pl.ds(i, QUERY_HEADS, stride=ROWS), :]
        q = jnp.where(own_group, jnp.concatenate([q] * KEY_VALUE_HEADS, axis=1), 0.0).astype(BF)
        pages = [table_ref[i, j] for j in range(SLOTS)]
        k = jnp.concatenate([keys[page] for page in pages], axis=0)
        scores = lax.dot_general(
            q, k, (((1,), (1,)), ((), ())), preferred_element_type=F32
        ) * (1.0 / math.sqrt(HEAD_DIM))
        scores = jnp.where(position < length_ref[i], scores, -1e30)
        peak = jnp.max(scores, axis=1, keepdims=True)
        powers = jnp.exp(scores - peak)
        total = jnp.sum(powers, axis=1, keepdims=True)
        v = jnp.concatenate([values[page] for page in pages], axis=0)
        mixed = jnp.dot(powers.astype(BF), v, preferred_element_type=F32)
        picked = jnp.zeros((QUERY_HEADS, HEAD_DIM), F32)
        for g in range(KEY_VALUE_HEADS):
            picked = jnp.where(group_of == g, mixed[:, g * HEAD_DIM : (g + 1) * HEAD_DIM], picked)
        part[pl.ds(i, QUERY_HEADS, stride=8), :] = picked
        part[pl.ds(ROWS + i, QUERY_HEADS, stride=8), :] = jnp.where(lane16 < 64, peak, total)

    def head_part(h):
        return part.at[pl.ds(pl.multiple_of(h * 8, 8), 8)]

    for d in range(1, SEQ):
        send(head_part(seq_peer(d)), part_buf.at[s], 3, {"seq": seq_peer(d)})
    part_buf[s] = part[pl.ds(pl.multiple_of(s * 8, 8), 8), :]
    whole(part_buf.at[pl.ds(0, SEQ - 1)], 3).wait_recv()
    lower = lane8 < 64
    joint = part_buf[0]
    for h in range(1, SEQ):
        joint = jnp.maximum(joint, part_buf[h])
    above = jnp.zeros((8, 128), F32)
    below = jnp.zeros((8, 128), F32)
    for h in range(SEQ):
        piece = part_buf[h]
        factor = jnp.exp(jnp.where((row8 >= ROWS) & lower, piece - joint, 0.0))
        factor = jnp.where(lower, factor, pltpu.roll(factor, 64, 1))
        below = below + factor * piece
        above = above + pltpu.roll(factor, ROWS, 0) * piece
    below = jnp.where(lower, pltpu.roll(below, 64, 1), below)
    below = pltpu.roll(below, ROWS, 0)
    attention = jnp.where(row8 < ROWS, above / jnp.where(row8 < ROWS, below, 1.0), 0.0).astype(BF)

    local[2].wait()
    whole(weights.at[pl.ds(0, EXPERTS - 1)], 2).wait_recv()
    for k in range(EXPERTS):
        columns = jnp.dot(attention, weights[k], preferred_element_type=F32)
        for side in range(2):
            proj[2 * k + side] = columns[:ROWS, side * FEATURES : (side + 1) * FEATURES]
    for d in range(1, SEQ):
        send(proj.at[seq_peer(d)], proj_buf.at[s], 4, {"seq": seq_peer(d)})
    proj_buf[s] = proj[s]
    whole(proj_buf.at[pl.ds(0, SEQ - 1)], 4).wait_recv()
    resid = proj_buf[0]
    for h in range(1, SEQ):
        resid = resid + proj_buf[h]
    resid = hidden_ref[...].astype(F32) + resid

    square = jnp.sum(resid * resid, axis=1, keepdims=True)
    high = square.astype(BF).astype(F32)
    tail = jnp.where(iota((ROWS, 128), 1) < 64, high, square - high)
    slabs[me, :, pl.ds(0, FEATURES)] = (resid * gain_ref[...]).astype(BF)
    slabs[me, :, pl.ds(FEATURES, 128)] = tail.astype(BF)
    for d in range(1, BATCHES * SEQ):
        peer = pair_peer(d)
        send(slabs.at[me], slabs.at[me], 5, {"batch": peer // SEQ, "seq": lax.rem(peer, SEQ)})
    whole(slabs.at[pl.ds(0, BATCHES * SEQ - 1)], 5).wait_recv()
    for block in range(BATCHES):
        squares = jnp.zeros((ROWS, 128), F32)
        for n in range(SEQ):
            squares = squares + slabs[block * SEQ + n, :, pl.ds(FEATURES, 128)].astype(F32)
        squares = squares + pltpu.roll(squares, 64, 1)
        scale = lax.rsqrt(squares / D + 1e-05)
        scale = jnp.concatenate([scale, scale], axis=1)
        for n in range(SEQ):
            row, column = ((n // 4) * BATCHES + block) * 8, (n % 4) * FEATURES
            tokens[pl.ds(row, ROWS), pl.ds(column, FEATURES)] = (
                slabs[block * SEQ + n, :, pl.ds(0, FEATURES)].astype(F32) * scale
            )

    whole(info.at[0], 1).wait_recv()
    facts = jnp.concatenate([info[0], info[1]] * 4, axis=0)
    row64, lane64 = iota((64, 128), 0), iota((64, 128), 1)
    same = (row64 // 16 == lane64 // 4 % 4) & (row64 // 8 % 2 == lane64 // 2 % 2)
    slot = (lane64 // 16 * 2 + lane64 % 2).astype(F32)
    hits = [same & (facts[:, k : k + 1] == slot) for k in range(2)]
    placing = jnp.where(hits[0] | hits[1], 1.0, 0.0).astype(BF)
    mixing = jnp.where(hits[0], facts[:, 2:3], 0.0) + jnp.where(hits[1], facts[:, 3:4], 0.0)
    placed = lax.dot_general(
        placing, tokens[...].astype(BF), (((0,), (0,)), ((), ())), preferred_element_type=F32
    ).astype(BF)
    for k in range(EXPERTS):
        sent[k] = placed[16 * k : 16 * (k + 1), :]
    for d in range(1, EXPERTS):
        send(sent.at[expert_peer(d)], slots.at[e], 6, {"expert": expert_peer(d)})
    slots[e] = sent[e]
    for copy in local[3:]:
        copy.wait()
    whole(slots.at[pl.ds(0, EXPERTS - 1)], 6).wait_recv()

    rows = slots[...].reshape(128, QUARTER)
    quarter_of = iota((128, QUARTER), 0) // 4 % 4
    gate_sum = jnp.zeros((128, HIDDEN), F32)
    up_sum = jnp.zeros((128, HIDDEN), F32)
    for n in range(4):
        mine = jnp.where(quarter_of == n, rows, jnp.zeros_like(rows))
        gate_sum += jnp.dot(mine, gate[pl.ds(n * QUARTER, QUARTER), :], preferred_element_type=F32)
        up_sum += jnp.dot(mine, up[pl.ds(n * QUARTER, QUARTER), :], preferred_element_type=F32)

    def folded(array):
        array = array.reshape(EXPERTS, 16, HIDDEN)
        array = array[:, :8] + array[:, 8:]
        return (array + pltpu.roll(array, 4, 1)).reshape(EXPERTS * 8, HIDDEN)

    gate_part, up_part = folded(gate_sum), folded(up_sum)
    act = (gate_part / (1.0 + jnp.exp(-gate_part)) * up_part).astype(BF)
    first = iota((64, QUARTER), 0) % 8 < 4
    halves = []
    for n in range(0, 4, 2):
        pair = [
            jnp.dot(act, down[:, pl.ds((n + m) * QUARTER, QUARTER)], preferred_element_type=F32)
            for m in range(2)
        ]
        halves.append(jnp.where(first, pair[0], pair[1]))
    for k in range(EXPERTS):
        returned[k] = jnp.concatenate(
            [half[8 * k : 8 * (k + 1)] for half in halves], axis=0
        ).astype(BF)
    for d in range(1, EXPERTS):
        send(returned.at[expert_peer(d)], results.at[e], 7, {"expert": expert_peer(d)})
    results[e] = returned[e]
    whole(results.at[pl.ds(0, EXPERTS - 1)], 7).wait_recv()

    found = results[...].reshape(128, QUARTER)
    rest = mixing
    merged = jnp.zeros((64, QUARTER), F32)
    for _ in range(3):
        top = rest.astype(BF)
        rest = rest - top.astype(F32)
        merged += jnp.dot(top, found, preferred_element_type=F32)
    for block in range(BATCHES):
        for n in range(SEQ):
            row, column = ((n // 4) * BATCHES + block) * 8, (n % 4) * FEATURES
            terms[block * SEQ + n] = merged[row : row + ROWS, column : column + FEATURES].astype(BF)
    for d in range(1, BATCHES * SEQ):
        peer = pair_peer(d)
        send(terms.at[peer], term_buf.at[me], 8, {"batch": peer // SEQ, "seq": lax.rem(peer, SEQ)})
    term_buf[me] = terms[me]
    whole(term_buf.at[pl.ds(0, BATCHES * SEQ - 1)], 8).wait_recv()
    expert_sum = jnp.zeros((ROWS, FEATURES), F32)
    for n in range(BATCHES * SEQ):
        expert_sum = expert_sum + term_buf[n].astype(F32)
    out_ref[...] = (resid + expert_sum).astype(BF)

    for phase, ref in enumerate((
        query_buf.at[pl.ds(0, SEQ - 1)], info.at[0], weights.at[pl.ds(0, EXPERTS - 1)],
        part_buf.at[pl.ds(0, SEQ - 1)], proj_buf.at[pl.ds(0, SEQ - 1)],
        slabs.at[pl.ds(0, BATCHES * SEQ - 1)], slots.at[pl.ds(0, EXPERTS - 1)],
        results.at[pl.ds(0, EXPERTS - 1)], term_buf.at[pl.ds(0, BATCHES * SEQ - 1)],
    )):
        whole(ref, phase).wait_send()


def per_device(
    hidden_state, queries, page_table, lengths, paged_keys, paged_values, out_weight, norm_gain,
    expert_ids, route_weights, expert_gate, expert_up, expert_down,
):
    vmem = pl.BlockSpec(memory_space=pltpu.VMEM)
    smem = pl.BlockSpec(memory_space=pltpu.SMEM)
    hbm = pl.BlockSpec(memory_space=pl.ANY)
    return pl.pallas_call(
        kernel,
        out_shape=jax.ShapeDtypeStruct((ROWS, FEATURES), BF),
        in_specs=[vmem, vmem, smem, smem, hbm, hbm, hbm, vmem, smem, smem, hbm, hbm, hbm],
        out_specs=vmem,
        scratch_shapes=[
            pltpu.VMEM((POOL, PAGE_TOKENS, 512), BF),
            pltpu.VMEM((POOL, PAGE_TOKENS, 512), BF),
            pltpu.VMEM((D, HIDDEN), BF),
            pltpu.VMEM((D, HIDDEN), BF),
            pltpu.VMEM((HIDDEN, D), BF),
            pltpu.VMEM((EXPERTS, HEAD_DIM, 512), BF),
            pltpu.VMEM((SEQ, ROWS, HEAD_DIM), BF),
            pltpu.VMEM((SEQ * ROWS, HEAD_DIM), F32),
            pltpu.VMEM((SEQ * 8, HEAD_DIM), F32),
            pltpu.VMEM((SEQ, 8, HEAD_DIM), F32),
            pltpu.VMEM((SEQ, ROWS, FEATURES), F32),
            pltpu.VMEM((SEQ, ROWS, FEATURES), F32),
            pltpu.VMEM((BATCHES, 8, 128), F32),
            pltpu.VMEM((BATCHES * SEQ, ROWS, FEATURES + 128), BF),
            pltpu.VMEM((64, QUARTER), F32),
            pltpu.VMEM((EXPERTS, 16, QUARTER), BF),
            pltpu.VMEM((EXPERTS, 16, QUARTER), BF),
            pltpu.VMEM((EXPERTS, 16, QUARTER), BF),
            pltpu.VMEM((EXPERTS, 16, QUARTER), BF),
            pltpu.VMEM((BATCHES * SEQ, ROWS, FEATURES), BF),
            pltpu.VMEM((BATCHES * SEQ, ROWS, FEATURES), BF),
            pltpu.SemaphoreType.DMA((6,)),
            pltpu.SemaphoreType.DMA((9,)),
            pltpu.SemaphoreType.DMA((9,)),
        ],
        compiler_params=pltpu.CompilerParams(collective_id=0, has_side_effects=True),
        name="layer",
    )(
        hidden_state, queries, page_table[:, 0], lengths, paged_keys[0], paged_values[0],
        out_weight, norm_gain[None], expert_ids, route_weights, expert_gate[0], expert_up[0],
        expert_down[0],
    )


def solution(mesh):
    rows = P(("batch", "expert"), "seq")
    pages = P(("batch", "expert"), "seq", None, None)
    in_specs = (
        rows, rows, P(("batch", "expert"), "seq", None), P(("batch", "expert")), pages, pages,
        P("seq", "expert"), P("seq"), P(("batch", "expert"), None), P(("batch", "expert"), None),
        P("expert", None, ("seq", "batch")), P("expert", None, ("seq", "batch")),
        P("expert", ("seq", "batch"), None),
    )
    return jax.shard_map(
        per_device, mesh=mesh, in_specs=in_specs, out_specs=rows, check_vma=False
    )
```

```python
import functools
import math

import jax
import jax.numpy as jnp
from jax import lax
from jax.experimental import pallas as pl
from jax.experimental.pallas import tpu as pltpu
from jax.sharding import PartitionSpec as P

D = 4096
QUERY_HEADS = 16
KEY_VALUE_HEADS = 4
HEAD_DIM = 128
PAGE_TOKENS = 128
SLOTS = 4
ROWS = 4
SEQ = 16
EXPERTS = 8
BATCHES = 2
POOL = 20
FEATURES = D // SEQ
HIDDEN = 256
QUARTER = D // 4
BF = jnp.bfloat16
F32 = jnp.float32
MESH = pl.DeviceIdType.MESH


def iota(shape, dim):
    return lax.broadcasted_iota(jnp.int32, shape, dim)


def kernel(
    hidden_hbm, query_hbm, table_hbm, length_hbm, keys_hbm, values_hbm, weight_hbm, gain_hbm,
    ids_hbm, route_hbm, gate_hbm, up_hbm, down_hbm, out_ref,
    hidden_ref, query_ref, gain_ref, table_ref, length_ref, ids_ref, route_ref,
    keys, values, gate, up, down, weights,
    query_buf, query_rows, part, part_buf, proj, proj_buf, info, gains, slabs, tokens, scales,
    sent, slots, scale_sent, scale_buf, scale_rows, frames, returned, results, terms, term_buf,
    local_sems, send_sems, recv_sems,
):
    s = lax.axis_index("seq")
    e = lax.axis_index("expert")
    b = lax.axis_index("batch")
    me = b * SEQ + s

    local = [
        pltpu.make_async_copy(source, target, local_sems.at[k])
        for k, (source, target) in enumerate((
            (query_hbm, query_ref), (ids_hbm, ids_ref), (route_hbm, route_ref),
            (gain_hbm, gain_ref), (weight_hbm, weights.at[e]), (table_hbm, table_ref),
            (length_hbm, length_ref), (keys_hbm, keys), (values_hbm, values),
            (hidden_hbm, hidden_ref), (gate_hbm, gate), (up_hbm, up),
            *((down_hbm.at[:, pl.ds(n * QUARTER, QUARTER)], down.at[n]) for n in range(4)),
        ))
    ]
    for copy in local:
        copy.start()

    def seq_peer(d):
        return lax.rem(s + d, SEQ)

    def expert_peer(d):
        return lax.rem(e + d, EXPERTS)

    def pair_peer(d):
        return lax.rem(me + d, BATCHES * SEQ)

    barrier = pltpu.get_barrier_semaphore()
    for d in range(1, SEQ):
        pl.semaphore_signal(barrier, 1, device_id={"seq": seq_peer(d)}, device_id_type=MESH)
    for d in range(1, EXPERTS):
        pl.semaphore_signal(barrier, 1, device_id={"expert": expert_peer(d)}, device_id_type=MESH)
    pl.semaphore_signal(barrier, 1, device_id={"batch": 1 - b}, device_id_type=MESH)

    for copy in local[:5]:
        copy.wait()

    ids = [[ids_ref[k, t] for k in range(2)] for t in range(ROWS)]
    row8, lane8 = iota((8, 128), 0), iota((8, 128), 1)
    slab = jnp.full((8, 128), -1.0, F32)
    for t in range(ROWS):
        for k in range(2):
            earlier = jnp.int32(0)
            for a in range(2 * t + k):
                earlier = earlier + jnp.where(ids[a // 2][a % 2] == ids[t][k], 1, 0)
            target = (ids[t][k] * 2 + earlier).astype(F32)
            slab = jnp.where((row8 == t) & (lane8 == k), target, slab)
            slab = jnp.where((row8 == t) & (lane8 == 2 + k), route_ref[k, t], slab)
    info[b] = slab
    tokens[...] = jnp.zeros_like(tokens)
    scales[...] = jnp.zeros_like(scales)
    query_buf[s] = query_ref[...]
    gains[s] = gain_ref[...]

    pl.semaphore_wait(barrier, SEQ - 1 + EXPERTS - 1 + 1)

    def send(source, target, phase, device, arrival=None):
        pltpu.make_async_remote_copy(
            src_ref=source, dst_ref=target, send_sem=send_sems.at[phase],
            recv_sem=recv_sems.at[phase if arrival is None else arrival],
            device_id=device, device_id_type=MESH,
        ).start()

    def whole(ref, phase, arrival=None):
        return pltpu.make_async_remote_copy(
            src_ref=ref, dst_ref=ref, send_sem=send_sems.at[phase],
            recv_sem=recv_sems.at[phase if arrival is None else arrival],
            device_id={"batch": 1 - b}, device_id_type=MESH,
        )

    for d in range(1, SEQ):
        send(query_ref, query_buf.at[s], 0, {"seq": seq_peer(d)})
    send(info.at[b], info.at[b], 1, {"batch": 1 - b})
    for d in range(1, SEQ):
        send(gain_ref, gains.at[s], 21, {"seq": seq_peer(d)})
    partner = e + 1 - 2 * lax.rem(e, 2)
    ahead, behind, across = expert_peer(2), expert_peer(6), expert_peer(4)
    send(weights.at[e], weights.at[e], 19, {"expert": ahead})
    send(weights.at[e], weights.at[e], 19, {"expert": behind})
    send(weights.at[e], weights.at[e], 2, {"expert": partner})

    for copy in local[5:9]:
        copy.wait()
    whole(query_buf.at[pl.ds(0, SEQ - 1)], 0).wait_recv()
    half = HEAD_DIM // 2
    whole(weights.at[pl.ds(0, 2)], 19).wait_recv()
    for source, target, start in ((behind, ahead, 0), (ahead, behind, half)):
        piece = weights.at[source, pl.ds(start, half)]
        send(piece, piece, 20, {"expert": target})
    for source in (behind, ahead):
        send(weights.at[source], weights.at[source], 2, {"expert": partner})
    for h in range(QUERY_HEADS):
        query_rows[pl.ds(ROWS * h, ROWS), :] = query_buf[h].astype(F32)
    width = KEY_VALUE_HEADS * HEAD_DIM
    own_group = iota((QUERY_HEADS, width), 1) // HEAD_DIM == iota((QUERY_HEADS, width), 0) // 4
    spot = iota((QUERY_HEADS, SLOTS * PAGE_TOKENS), 1)
    position = (spot // PAGE_TOKENS * SEQ + s) * PAGE_TOKENS + spot % PAGE_TOKENS
    group_of = iota((QUERY_HEADS, HEAD_DIM), 0) // 4
    lane16 = iota((QUERY_HEADS, HEAD_DIM), 1)
    for i in range(ROWS):
        q = query_rows[pl.ds(i, QUERY_HEADS, stride=ROWS), :]
        q = jnp.where(own_group, jnp.concatenate([q] * KEY_VALUE_HEADS, axis=1), 0.0).astype(BF)
        pages = [table_ref[i, j] for j in range(SLOTS)]
        k = jnp.concatenate([keys[page] for page in pages], axis=0)
        scores = lax.dot_general(
            q, k, (((1,), (1,)), ((), ())), preferred_element_type=F32
        ) * (1.0 / math.sqrt(HEAD_DIM))
        scores = jnp.where(position < length_ref[i], scores, -1e30)
        peak = jnp.max(scores, axis=1, keepdims=True)
        powers = jnp.exp(scores - peak)
        total = jnp.sum(powers, axis=1, keepdims=True)
        v = jnp.concatenate([values[page] for page in pages], axis=0)
        mixed = jnp.dot(powers.astype(BF), v, preferred_element_type=F32)
        picked = jnp.zeros((QUERY_HEADS, HEAD_DIM), F32)
        for g in range(KEY_VALUE_HEADS):
            picked = jnp.where(group_of == g, mixed[:, g * HEAD_DIM : (g + 1) * HEAD_DIM], picked)
        part[pl.ds(i, QUERY_HEADS, stride=8), :] = picked
        part[pl.ds(ROWS + i, QUERY_HEADS, stride=8), :] = jnp.where(lane16 < 64, peak, total)

    def head_part(h):
        return part.at[pl.ds(pl.multiple_of(h * 8, 8), 8)]

    for d in range(1, SEQ):
        send(head_part(seq_peer(d)), part_buf.at[s], 3, {"seq": seq_peer(d)})
    part_buf[s] = part[pl.ds(pl.multiple_of(s * 8, 8), 8), :]
    whole(weights.at[0], 20).wait_recv()
    send(weights.at[across], weights.at[across], 2, {"expert": partner})
    whole(part_buf.at[pl.ds(0, SEQ - 1)], 3).wait_recv()
    lower = lane8 < 64
    joint = part_buf[0]
    for h in range(1, SEQ):
        joint = jnp.maximum(joint, part_buf[h])
    above = jnp.zeros((8, 128), F32)
    below = jnp.zeros((8, 128), F32)
    for h in range(SEQ):
        piece = part_buf[h]
        factor = jnp.exp(jnp.where((row8 >= ROWS) & lower, piece - joint, 0.0))
        factor = jnp.where(lower, factor, pltpu.roll(factor, 64, 1))
        below = below + factor * piece
        above = above + pltpu.roll(factor, ROWS, 0) * piece
    below = jnp.where(lower, pltpu.roll(below, 64, 1), below)
    below = pltpu.roll(below, ROWS, 0)
    attention = jnp.where(row8 < ROWS, above / jnp.where(row8 < ROWS, below, 1.0), 0.0).astype(BF)

    whole(weights.at[pl.ds(0, 4)], 2).wait_recv()
    for copy in local[9:10]:
        copy.wait()
    for k in range(EXPERTS):
        columns = jnp.dot(attention, weights[k], preferred_element_type=F32)
        for side in range(2):
            proj[2 * k + side] = columns[:ROWS, side * FEATURES : (side + 1) * FEATURES]
    for d in range(1, SEQ):
        send(proj.at[seq_peer(d)], proj_buf.at[s], 4, {"seq": seq_peer(d)})
    proj_buf[s] = proj[s]
    whole(proj_buf.at[pl.ds(0, SEQ - 1)], 4).wait_recv()
    resid = proj_buf[0]
    for h in range(1, SEQ):
        resid = resid + proj_buf[h]
    resid = hidden_ref[...].astype(F32) + resid

    y, depth = s // 4, b * 4 + lax.rem(s, 4)

    def quarter(d):
        return lax.rem(y + d, 4)

    def column_peer(dy, dz):
        far = lax.rem(depth + dz, 8)
        return quarter(dy), far, {"batch": far // 4, "seq": quarter(dy) * 4 + lax.rem(far, 4)}

    slabs[me] = resid.astype(BF)
    for dy in (2, 1, 3, 0):
        for dz in (4, 3, 5, 2, 6, 1, 7, 0):
            if dy or dz:
                device = column_peer(dy, dz)[2]
                send(slabs.at[me], slabs.at[me], 5, device, 5 + y)
    whole(info.at[0], 1).wait_recv()
    whole(gains.at[pl.ds(0, SEQ - 1)], 21).wait_recv()
    facts = jnp.concatenate([info[0], info[1]], axis=0)
    row16, lane = iota((16, 128), 0), iota((16, 128), 1)

    def hits(stride):
        slot = (lane // stride * 2 + lane % 2).astype(F32)
        same = (row16 // 8 == lane // 2 % 2) & (lane % stride < 4)
        return [same & (facts[:, k : k + 1] == slot) for k in range(2)]

    placed, found = hits(8), hits(4)
    placing = jnp.where(placed[0] | placed[1], 1.0, 0.0).astype(BF)[:, :64]
    rest = jnp.where(found[0], facts[:, 2:3], 0.0) + jnp.where(found[1], facts[:, 3:4], 0.0)

    def three_parts(array):
        parts = []
        for _ in range(3):
            parts.append(array.astype(BF))
            array = array - parts[-1].astype(F32)
        return parts

    mixing = jnp.concatenate(three_parts(rest), axis=0)[:, :32]
    forth, back = (0, 1, 3, 2), (2, 1, 3, 0)
    squares = [jnp.zeros((ROWS, FEATURES), F32) for _ in range(BATCHES)]
    for k, d in enumerate(forth):
        count = 8 if d else 7
        whole(slabs.at[pl.ds(0, count)], 5, 5 + quarter(d)).wait_recv()
        for block in range(BATCHES):
            for n in range(4):
                source = quarter(d) * 4 + n
                piece = slabs[block * SEQ + source].astype(F32)
                squares[block] = squares[block] + piece * piece
                tokens[k, pl.ds(block * 8, ROWS), pl.ds(n * FEATURES, FEATURES)] = (
                    piece * gains[source]
                )
        rows = lax.dot_general(
            placing, tokens[k].astype(BF), (((0,), (0,)), ((), ())), preferred_element_type=F32
        )
        for n in range(EXPERTS):
            sent[k, n] = rows[8 * n : 8 * n + ROWS].astype(BF)
        for n in range(1, EXPERTS):
            peer = expert_peer(n)
            send(sent.at[k, peer], slots.at[k, e], 9, {"expert": peer}, 9 + k)
        slots[k, e] = sent[k, e]
    for block in range(BATCHES):
        mean = jnp.sum(squares[block], axis=1, keepdims=True) / D
        scales[pl.ds(block * 8, ROWS), :] = jnp.broadcast_to(
            lax.rsqrt(mean + 1e-05), (ROWS, 128)
        )
    rows = jnp.zeros((64, 128), F32)
    for piece in three_parts(scales[...]):
        rows += lax.dot_general(
            placing, piece, (((0,), (0,)), ((), ())), preferred_element_type=F32
        )
    for n in range(EXPERTS):
        scale_sent[n] = rows[8 * n : 8 * n + ROWS]
    for n in range(1, EXPERTS):
        peer = expert_peer(n)
        send(scale_sent.at[peer], scale_buf.at[e], 13, {"expert": peer})
    scale_buf[e] = scale_sent[e]

    for copy in local[10:]:
        copy.wait()
    gate_sum = jnp.zeros((32, HIDDEN), F32)
    up_sum = jnp.zeros((32, HIDDEN), F32)
    for k, d in enumerate(forth):
        whole(slots.at[k, pl.ds(0, EXPERTS - 1)], 9, 9 + k).wait_recv()
        for n in range(EXPERTS):
            frames[k, pl.ds(n * ROWS, ROWS), :] = slots[k, n].astype(F32)
        rows = frames[k].astype(BF)
        window = pl.ds(pl.multiple_of(quarter(d) * QUARTER, QUARTER), QUARTER)
        gate_sum += jnp.dot(rows, gate[window, :], preferred_element_type=F32)
        up_sum += jnp.dot(rows, up[window, :], preferred_element_type=F32)
    whole(scale_buf.at[pl.ds(0, EXPERTS - 1)], 13).wait_recv()
    for n in range(EXPERTS):
        scale_rows[pl.ds(n * ROWS, ROWS), :] = scale_buf[n]
    scale = jnp.concatenate([scale_rows[...]] * 2, axis=1)
    gate_part, up_part = gate_sum * scale, up_sum * scale
    act = (gate_part / (1.0 + jnp.exp(-gate_part)) * up_part).astype(BF)
    for k, d in enumerate(back):
        rows = jnp.dot(act, down[quarter(d)], preferred_element_type=F32)
        for n in range(EXPERTS):
            returned[k, n] = rows[ROWS * n : ROWS * (n + 1)].astype(BF)
        for n in range(1, EXPERTS):
            peer = expert_peer(n)
            send(returned.at[k, peer], results.at[k, e], 14, {"expert": peer}, 14 + k)
        results[k, e] = returned[k, e]
    for k, d in enumerate(back):
        whole(results.at[k, pl.ds(0, EXPERTS - 1)], 14, 14 + k).wait_recv()
        for n in range(EXPERTS):
            frames[k, pl.ds(n * ROWS, ROWS), :] = results[k, n].astype(F32)
        rows = jnp.dot(mixing, frames[k].astype(BF), preferred_element_type=F32)
        rows = rows[:16] + rows[16:32] + rows[32:]
        for n in range(8):
            terms[k, n] = rows[
                n // 4 * 8 : n // 4 * 8 + ROWS, n % 4 * FEATURES : (n % 4 + 1) * FEATURES
            ].astype(BF)
        for dz in (4, 3, 5, 2, 6, 1, 7, 0):
            if d or dz:
                _, far, device = column_peer(d, dz)
                send(terms.at[k, far], term_buf.at[me], 18, device)
    term_buf[me] = terms[3, depth]
    whole(term_buf.at[pl.ds(0, BATCHES * SEQ - 1)], 18).wait_recv()
    expert_sum = jnp.zeros((ROWS, FEATURES), F32)
    for n in range(BATCHES * SEQ):
        expert_sum = expert_sum + term_buf[n].astype(F32)
    out_ref[...] = resid + expert_sum

    for phase, ref in (
        (0, query_buf.at[pl.ds(0, SEQ - 1)]), (1, info.at[0]), (2, weights.at[pl.ds(0, 4)]),
        (3, part_buf.at[pl.ds(0, SEQ - 1)]), (4, proj_buf.at[pl.ds(0, SEQ - 1)]),
        (5, slabs.at[pl.ds(0, BATCHES * SEQ - 1)]), (9, slots.at[:, pl.ds(0, EXPERTS - 1)]),
        (13, scale_buf.at[pl.ds(0, EXPERTS - 1)]), (14, results.at[:, pl.ds(0, EXPERTS - 1)]),
        (18, term_buf.at[pl.ds(0, BATCHES * SEQ - 1)]), (19, weights.at[pl.ds(0, 2)]),
        (20, weights.at[0]), (21, gains.at[pl.ds(0, SEQ - 1)]),
    ):
        whole(ref, phase).wait_send()


def per_device(
    hidden_state, queries, page_table, lengths, paged_keys, paged_values, out_weight, norm_gain,
    expert_ids, route_weights, expert_gate, expert_up, expert_down,
):
    hbm = pl.BlockSpec(memory_space=pltpu.HBM)
    result = pl.pallas_call(
        kernel,
        out_shape=jax.ShapeDtypeStruct((ROWS, FEATURES), F32),
        in_specs=[hbm] * 13,
        out_specs=pl.BlockSpec(memory_space=pltpu.VMEM),
        scratch_shapes=[
            pltpu.VMEM((ROWS, FEATURES), BF),
            pltpu.VMEM((ROWS, HEAD_DIM), BF),
            pltpu.VMEM((1, FEATURES), F32),
            pltpu.SMEM((ROWS, SLOTS), jnp.int32),
            pltpu.SMEM((ROWS,), jnp.int32),
            pltpu.SMEM((2, ROWS), jnp.int32),
            pltpu.SMEM((2, ROWS), F32),
            pltpu.VMEM((POOL, PAGE_TOKENS, 512), BF),
            pltpu.VMEM((POOL, PAGE_TOKENS, 512), BF),
            pltpu.VMEM((D, HIDDEN), BF),
            pltpu.VMEM((D, HIDDEN), BF),
            pltpu.VMEM((4, HIDDEN, QUARTER), BF),
            pltpu.VMEM((EXPERTS, HEAD_DIM, 512), BF),
            pltpu.VMEM((SEQ, ROWS, HEAD_DIM), BF),
            pltpu.VMEM((SEQ * ROWS, HEAD_DIM), F32),
            pltpu.VMEM((SEQ * 8, HEAD_DIM), F32),
            pltpu.VMEM((SEQ, 8, HEAD_DIM), F32),
            pltpu.VMEM((SEQ, ROWS, FEATURES), F32),
            pltpu.VMEM((SEQ, ROWS, FEATURES), F32),
            pltpu.VMEM((BATCHES, 8, 128), F32),
            pltpu.VMEM((SEQ, 1, FEATURES), F32),
            pltpu.VMEM((BATCHES * SEQ, ROWS, FEATURES), BF),
            pltpu.VMEM((4, 16, QUARTER), F32),
            pltpu.VMEM((16, 128), F32),
            pltpu.VMEM((4, EXPERTS, ROWS, QUARTER), BF),
            pltpu.VMEM((4, EXPERTS, ROWS, QUARTER), BF),
            pltpu.VMEM((EXPERTS, ROWS, 128), F32),
            pltpu.VMEM((EXPERTS, ROWS, 128), F32),
            pltpu.VMEM((32, 128), F32),
            pltpu.VMEM((4, 32, QUARTER), F32),
            pltpu.VMEM((4, EXPERTS, ROWS, QUARTER), BF),
            pltpu.VMEM((4, EXPERTS, ROWS, QUARTER), BF),
            pltpu.VMEM((4, 8, ROWS, FEATURES), BF),
            pltpu.VMEM((BATCHES * SEQ, ROWS, FEATURES), BF),
            pltpu.SemaphoreType.DMA((16,)),
            pltpu.SemaphoreType.DMA((22,)),
            pltpu.SemaphoreType.DMA((22,)),
        ],
        compiler_params=pltpu.CompilerParams(collective_id=0, has_side_effects=True),
        name="layer",
    )(
        hidden_state, queries, page_table[:, 0], lengths, paged_keys[0], paged_values[0],
        out_weight, norm_gain[None], expert_ids.T, route_weights.T, expert_gate[0], expert_up[0],
        expert_down[0],
    )
    return result.astype(BF)


def solution(mesh):
    rows = P(("batch", "expert"), "seq")
    pages = P(("batch", "expert"), "seq", None, None)
    in_specs = (
        rows, rows, P(("batch", "expert"), "seq", None), P(("batch", "expert")), pages, pages,
        P("seq", "expert"), P("seq"), P(("batch", "expert"), None), P(("batch", "expert"), None),
        P("expert", None, ("seq", "batch")), P("expert", None, ("seq", "batch")),
        P("expert", ("seq", "batch"), None),
    )
    return jax.shard_map(
        per_device, mesh=mesh, in_specs=in_specs, out_specs=rows, check_vma=False
    )
```
